32 devices in a mesh: mem: 2 (over y), lat: 4 (over z), lon: 4 (over x, core).
Axes of the slice: x: 2, y: 2, z: 4, core: 2. Of those that a mesh axis runs over, the one named last changes fastest.
Arguments:
- control: bfloat16 [62, 3, 4, 4, 73728], P('mem', None, 'lat', 'lon'), may hold values from -6 to 6
- perturbs: bfloat16 [62, 3, 4, 4, 73728], P('mem', None, 'lat', 'lon'), may hold values from -0.75 to 0.75
- static_input: bfloat16 [3, 4, 4, 73728], P(None, 'lat', 'lon'), may hold values from -6 to 6
- lat_basis: bfloat16 [768, 384], replicated, may hold values from -0.21875 to 0.21875
- local_spectrum: float32 [384, 768], P(None, 'lat'), may hold values from 0.1 to 1
- static_spectrum: float32 [384, 768], P(None, 'lat'), may hold values from 0.1 to 1
- static_weight: float32 [3], replicated, may hold values from 0.2 to 0.8
Outputs:
- increment: float32 [3, 4, 4, 73728], P(None, 'lat', 'lon')
The draws below stay inside these ranges and needn't reach their ends.
All inputs are finite; a program needn't handle non-finite values.
Results may differ from the reference program's by a relative error of at most 0.0073.
Values may be sent and summed in bfloat16 or wider, within the bound.
A program may use at most 128 MiB of HBM per device.

```python
import math
import jax
import jax.numpy as jnp
from jax import lax

NLON = 1536
NLAT = 768
KLON = 768
KLAT = 384
LEV = 3
MEMBERS = 62
CELLS = 73728
N_LAT = 4
N_LON = 4


def block_levels(own_key, shape, cuts, low, high):
    factor_of, own = 1.0, jax.random.fold_in(own_key, 6)
    for axis_at, parts in cuts:
        heights = jnp.exp(jax.random.uniform(jax.random.fold_in(own, axis_at), (parts,), jnp.float32, low / len(cuts), high / len(cuts)))
        factor_of = factor_of * jnp.repeat(heights, shape[axis_at] // parts).reshape([-1 if axis == axis_at else 1 for axis in range(len(shape))])
    return factor_of


def gaussian(own_key, dims, scale, limit, shards=(), held_as=jnp.bfloat16):
    result = jax.random.normal(own_key, dims, jnp.float32) * scale
    if len(shards) > 0:
        result = block_levels(own_key, dims, shards, -0.22, 0.18) * result
    return jnp.clip(result, min=-limit, max=limit).astype(held_as)


def setup_inputs(seed: int = 0) -> dict:
    arg_keys = jax.random.split(jax.random.key(seed), 8)
    control = gaussian(arg_keys[0], (MEMBERS, LEV, N_LAT, N_LON, CELLS), 1.0, 6.0, ((0, 2), (2, 4), (3, 4)))
    perturbs = gaussian(arg_keys[1], (MEMBERS, LEV, N_LAT, N_LON, CELLS), 0.125, 0.75, ((0, 2), (2, 4), (3, 4)))
    static_input = gaussian(arg_keys[2], (LEV, N_LAT, N_LON, CELLS), 1.0, 6.0, ((1, 4), (2, 4)))
    lat_basis = gaussian(arg_keys[3], (NLAT, KLAT), NLAT ** -0.5, 0.21875)
    local_spectrum = jnp.clip(jnp.exp(math.log(1.0) - 2.3025851 * jax.random.uniform(arg_keys[4], (KLAT, KLON), jnp.float32) ** block_levels(arg_keys[4], (KLAT, KLON), ((1, 4),), -0.2, 0.2)), 0.1, 1.0)
    static_spectrum = jnp.clip(jnp.exp(math.log(1.0) - 2.3025851 * jax.random.uniform(arg_keys[5], (KLAT, KLON), jnp.float32) ** block_levels(arg_keys[5], (KLAT, KLON), ((1, 4),), -0.2, 0.2)), 0.1, 1.0)
    static_weight = jnp.clip(jax.random.uniform(arg_keys[6], (LEV,), jnp.float32, 0.2, 0.8), 0.2, 0.8)
    return dict(control=control, perturbs=perturbs, static_input=static_input, lat_basis=lat_basis, local_spectrum=local_spectrum, static_spectrum=static_spectrum, static_weight=static_weight)


def zonal_table():
    half = KLON // 2
    points = jnp.arange(NLON, dtype=jnp.int32)
    column = jnp.arange(KLON, dtype=jnp.int32)
    wave = jnp.where(column < half, column, column - half + 1)
    phase = points[:, None] * wave[None, :] % NLON
    angle = 2.0 * jnp.pi / NLON * phase.astype(jnp.float32)
    scale = jnp.sqrt(jnp.float32(2.0 / NLON))
    values = jnp.where(column[None, :] < half, jnp.cos(angle), jnp.sin(angle)) * scale
    return values.astype(jnp.bfloat16)

def to_plain(blocks):
    lead = blocks.shape[:-3]
    count = len(lead)
    lat_rows = NLAT // N_LAT
    lon_cols = NLON // N_LON
    shaped = blocks.reshape(lead + (N_LAT, N_LON, lat_rows, lon_cols))
    shaped = jnp.moveaxis(shaped, count + 2, count + 1)
    return shaped.reshape(lead + (NLAT, NLON))

def to_blocks(plain):
    lead = plain.shape[:-2]
    count = len(lead)
    lat_rows = NLAT // N_LAT
    lon_cols = NLON // N_LON
    shaped = plain.reshape(lead + (N_LAT, lat_rows, N_LON, lon_cols))
    shaped = jnp.moveaxis(shaped, count + 1, count + 2)
    return shaped.reshape(lead + (N_LAT, N_LON, lat_rows * lon_cols))

def filter_fields(fields, spectrum, zonal, merid):
    zonal_f = zonal.astype(jnp.float32)
    merid_f = merid.astype(jnp.float32)
    waves = jnp.einsum('lyn,nk->lyk', fields.astype(jnp.float32), zonal_f).astype(jnp.bfloat16)
    coef = jnp.einsum('lyk,yj->ljk', waves.astype(jnp.float32), merid_f) * spectrum[None]
    scaled = coef.astype(jnp.bfloat16)
    back = jnp.einsum('ljk,yj->lyk', scaled.astype(jnp.float32), merid_f).astype(jnp.bfloat16)
    grid = jnp.einsum('lyk,nk->lyn', back.astype(jnp.float32), zonal_f).astype(jnp.bfloat16)
    return grid

def reference(control, perturbs, static_input, lat_basis, local_spectrum, static_spectrum, static_weight):
    zonal = zonal_table()

    def add_member(total, pair):
        alpha, pert = pair
        grid = filter_fields(to_plain(alpha), local_spectrum, zonal, lat_basis)
        return (total + to_plain(pert).astype(jnp.float32) * grid.astype(jnp.float32), None)
    start = jnp.zeros((LEV, NLAT, NLON), jnp.float32)
    ensemble, unused = lax.scan(add_member, start, (control, perturbs))
    static_part = filter_fields(to_plain(static_input), static_spectrum, zonal, lat_basis).astype(jnp.float32)
    weight = static_weight[:, None, None]
    return to_blocks(weight * static_part + (1.0 - weight) * ensemble)
```

```python
import functools

import jax
import jax.numpy as jnp
import numpy as np
from jax import lax
from jax.experimental import pallas as pl
from jax.experimental.pallas import tpu as pltpu
from jax.sharding import PartitionSpec as P

NLON = 1536
NLAT = 768
KLON = 768
LANES = 128
HALF = 64
GROUP = 8
STEP_ROWS = 32
AHEAD = 4
MESH = pl.DeviceIdType.MESH
F32, BF16 = jnp.float32, jnp.bfloat16


def zonal_table():
    half = KLON // 2
    column = np.arange(KLON)
    wave = np.where(column < half, column, column - half + 1)
    angle = 2.0 * np.pi / NLON * (np.arange(NLON)[:, None] * wave[None, :] % NLON)
    values = np.where(column[None, :] < half, np.cos(angle), np.sin(angle))
    return (np.sqrt(2.0 / NLON) * values).astype(jnp.bfloat16)


def packed_table(n_lat):
    blocks = zonal_table().reshape(NLON, n_lat, KLON // n_lat)
    main = blocks[:, :, :LANES].reshape(NLON, -1)
    rest = blocks[:, :, LANES:]
    swapped = rest.reshape(NLON, n_lat // 2, 2, HALF)[:, :, ::-1]
    return np.concatenate([main, rest.reshape(NLON, -1), swapped.reshape(NLON, -1)], 1)


def aligned(start, to):
    return pl.multiple_of(start, to)


def kernel(
    sizes,
    ctrl, ctrl_last, pert, pert_last, table_in, merid_in, merid_t_in, spec_in, weight,
    out,
    xin, wst, zin, bin_, gin, table, merid, merid_t, spec,
    scaled, rows_in, waves, rows_out, grid, pbuf, part, peer,
    csem, xs, xr, zs, zr, bs, br, gs, gr, ms, mr, ps,
):
    levels, n_lat, n_lon, rows, cols, step = sizes
    blocks = rows // step
    chunks = levels * blocks
    width = step * cols
    pair = 3 * LANES
    pairs = GROUP // 2
    rest_a = n_lat * LANES
    rest_b = rest_a + n_lat * HALF
    my_mem, my_lat, my_lon = lax.axis_index("mem"), lax.axis_index("lat"), lax.axis_index("lon")
    lon_order = [2, 3, 1] if n_lon == 4 else list(range(1, n_lon))
    lat_order = [2, 3, 1] if n_lat == 4 else list(range(1, n_lat))

    def at_lon(lon):
        return (my_mem, my_lat, lon)

    def at_lat(lat):
        return (my_mem, lat, my_lon)

    def split(c):
        return lax.div(c, blocks), lax.rem(c, blocks)

    def cells(b):
        return pl.ds(aligned(b * width, LANES), width)

    def band(b):
        return pl.ds(aligned(b * step, 16), step)

    def remote(src, dst, send, recv, device):
        pltpu.make_async_remote_copy(
            src_ref=src, dst_ref=dst, send_sem=send, recv_sem=recv,
            device_id=device, device_id_type=MESH,
        ).start()

    def wait(ref, sem):
        pltpu.make_async_copy(ref, ref, sem).wait()

    consts = [(table_in, table), (merid_in, merid), (merid_t_in, merid_t), (spec_in, spec)]
    for i, (src, dst) in enumerate(consts):
        pltpu.make_async_copy(src, dst, csem.at[i]).start()

    barrier = pltpu.get_barrier_semaphore()
    for s in range(1, n_lon):
        pl.semaphore_signal(barrier, 1, device_id=at_lon(my_lon ^ s), device_id_type=MESH)
    for s in range(1, n_lat):
        pl.semaphore_signal(barrier, 1, device_id=at_lat(my_lat ^ s), device_id_type=MESH)
    mem_peer = (1 - my_mem, my_lat, my_lon)
    pl.semaphore_signal(barrier, 1, device_id=mem_peer, device_id_type=MESH)
    pl.semaphore_wait(barrier, n_lon + n_lat - 1)

    def send_strips(c):
        lv, b = split(c)
        dst = xin.at[lv, my_lon, :, cells(b)]

        def each(lon, go):
            @pl.when(lon < n_lon - 1)
            def _():
                go(ctrl.at[lv, pl.ds(aligned(lon * GROUP, GROUP), GROUP), cells(b)])

            @pl.when(lon == n_lon - 1)
            def _():
                go(ctrl_last.at[lv, :, cells(b)])

        for s in lon_order:
            lon = my_lon ^ s
            each(lon, lambda src, lon=lon: remote(src, dst, xs.at[c], xr.at[c], at_lon(lon)))
        each(my_lon, lambda src: pltpu.make_async_copy(src, dst, xr.at[c]).start())

    def load_perturbs(c):
        lv, b = split(c)
        slot = lax.rem(c, 2)
        for e in range(n_lon - 1):
            pltpu.make_async_copy(
                pert.at[lv, pl.ds(e * GROUP, GROUP), cells(b)], pbuf.at[slot, e], ps.at[slot]
            ).start()
        pltpu.make_async_copy(
            pert_last.at[lv, :, cells(b)], pbuf.at[slot, n_lon - 1], ps.at[slot]
        ).start()

    for c in range(min(AHEAD, chunks)):
        send_strips(c)
    load_perturbs(0)
    for i, (src, dst) in enumerate(consts):
        pltpu.make_async_copy(src, dst, csem.at[i]).wait()

    low = lax.broadcasted_iota(jnp.int32, (step, LANES), 1) < HALF
    low_16 = low.astype(F32).astype(BF16)
    high_16 = (1.0 - low.astype(F32)).astype(BF16)

    def forward(c):
        lv, b = split(c)
        wait(xin.at[lv, :, :, cells(b)], xr.at[c])

        def two_rows(i, carry):
            for e in range(n_lon):
                at = pl.ds(aligned(b * width + i * (2 * cols), LANES), 2 * cols)
                x = xin[lv, e, :, at].astype(F32)
                x = jnp.concatenate([x[:, :cols], x[:, cols:]], 0).astype(BF16)
                rows_in[pl.ds(aligned(i * 16, 16), 16), e * cols : (e + 1) * cols] = x
            return carry

        lax.fori_loop(0, step // 2, two_rows, 0)
        for k in range(0, waves.shape[0], 2):
            at = slice(k * LANES, (k + 2) * LANES)
            pair_k = jnp.dot(rows_in[...], table[:, at], preferred_element_type=F32)
            waves[k] = pair_k[:, :LANES]
            waves[k + 1] = pair_k[:, LANES:]
        for p in range(pairs):
            for d in range(n_lat):
                main = d
                in_a = rest_a // LANES + d // 2
                in_b = rest_b // LANES + d // 2
                first, second = (in_a, in_b) if d % 2 == 0 else (in_b, in_a)
                even, odd = pl.ds(2 * p, step, GROUP), pl.ds(2 * p + 1, step, GROUP)
                last = jnp.where(low, waves[first, even, :], waves[second, odd, :])
                at = p * pair
                wst[lv, d, band(b), at : at + LANES] = waves[main, even, :].astype(BF16)
                wst[lv, d, band(b), at + LANES : at + 2 * LANES] = waves[main, odd, :].astype(BF16)
                wst[lv, d, band(b), at + 2 * LANES : at + pair] = last.astype(BF16)
        dst = zin.at[lv, my_lat, band(b), :]
        for s in lat_order:
            lat = my_lat ^ s
            remote(wst.at[lv, lat, band(b), :], dst, zs.at[c], zr.at[c], at_lat(lat))
        pltpu.make_async_copy(wst.at[lv, my_lat, band(b), :], dst, zr.at[c]).start()

    def spectral(lv):
        def arrived(b, carry):
            wait(zin.at[lv, :, band(b), :], zr.at[lv * blocks + b])
            return carry

        lax.fori_loop(0, blocks, arrived, 0)
        for p in range(pairs):
            at = slice(p * pair, (p + 1) * pair)
            columns = zin[lv, :, :, at].reshape(n_lat * rows, pair)
            coef = jnp.dot(merid_t[...], columns, preferred_element_type=F32)
            kind = 1 if p == pairs - 1 else 0
            scaled[:, at] = (coef * spec[kind]).astype(BF16)

    def backward(c):
        lv, b = split(c)
        lhs = jnp.concatenate([merid[d, band(b), :] for d in range(n_lat)], 0)
        for p in range(pairs):
            at = slice(p * pair, (p + 1) * pair)
            back = jnp.dot(lhs, scaled[:, at], preferred_element_type=F32).astype(BF16)
            for d in range(n_lat):
                zin[lv, d, band(b), at] = back[d * step : (d + 1) * step]
        dst = bin_.at[lv, my_lat, band(b), :]
        for s in lat_order:
            lat = my_lat ^ s
            remote(zin.at[lv, lat, band(b), :], dst, bs.at[c], br.at[c], at_lat(lat))
        pltpu.make_async_copy(zin.at[lv, my_lat, band(b), :], dst, br.at[c]).start()

    def to_grid(c):
        lv, b = split(c)
        wait(bin_.at[lv, :, band(b), :], br.at[c])
        for p in range(pairs):
            even = slice(2 * p * step, (2 * p + 1) * step)
            odd = slice((2 * p + 1) * step, (2 * p + 2) * step)
            at = p * pair
            for s in range(n_lat):
                main = slice(s * LANES, (s + 1) * LANES)
                in_a = slice(rest_a + s // 2 * LANES, rest_a + (s // 2 + 1) * LANES)
                in_b = slice(rest_b + s // 2 * LANES, rest_b + (s // 2 + 1) * LANES)
                first, second = (in_a, in_b) if s % 2 == 0 else (in_b, in_a)
                rest = bin_[lv, s, band(b), at + 2 * LANES : at + pair]
                rows_out[even, main] = bin_[lv, s, band(b), at : at + LANES]
                rows_out[odd, main] = bin_[lv, s, band(b), at + LANES : at + 2 * LANES]
                rows_out[even, first] = rest * low_16
                rows_out[odd, second] = rest * high_16
        for e in range(n_lon):
            part_e = lax.dot_general(
                rows_out[...], table[e * cols : (e + 1) * cols, :],
                (((1,), (1,)), ((), ())), preferred_element_type=F32,
            )
            for m in range(GROUP):
                for j in range(cols // LANES):
                    tile = part_e[m * step : (m + 1) * step, j * LANES : (j + 1) * LANES]
                    grid[e % 2, j, pl.ds(m, step, GROUP), :] = tile

            def two_rows(i, carry):
                x = [
                    grid[e % 2, j, pl.ds(aligned(i * 16 + h, GROUP), GROUP), :]
                    for h in (0, GROUP)
                    for j in range(cols // LANES)
                ]
                x = jnp.concatenate(x, 1).astype(BF16)
                at = pl.ds(aligned(b * width + i * (2 * cols), LANES), 2 * cols)
                xin[lv, e, :, at] = x
                return carry

            lax.fori_loop(0, step // 2, two_rows, 0)
        dst = gin.at[lv, my_lon, :, cells(b)]
        for s in lon_order:
            lon = my_lon ^ s
            remote(xin.at[lv, lon, :, cells(b)], dst, gs.at[c], gr.at[c], at_lon(lon))
        pltpu.make_async_copy(xin.at[lv, my_lon, :, cells(b)], dst, gr.at[c]).start()

    owns = jnp.where(my_mem == 0, 1.0, 0.0).astype(F32)
    is_static = lax.broadcasted_iota(jnp.int32, (GROUP, cols), 0) == GROUP - 1

    def gather_sum(c):
        lv, b = split(c)
        slot = lax.rem(c, 2)
        wait(pbuf.at[slot], ps.at[slot])

        @pl.when(c + 1 < chunks)
        def _():
            load_perturbs(c + 1)

        wait(gin.at[lv, :, :, cells(b)], gr.at[c])
        w = weight[lv]

        def eight_rows(i, carry):
            sums = []
            for y in range(GROUP):
                off = aligned(i * (GROUP * cols) + y * cols, LANES)
                total = jnp.zeros((GROUP, cols), F32)
                for e in range(n_lon):
                    at = pl.ds(aligned(b * width + off, LANES), cols)
                    field = gin[lv, e, :, at].astype(F32)
                    factor = pbuf[slot, e, :, pl.ds(off, cols)].astype(F32) * (1.0 - w)
                    if e == n_lon - 1:
                        factor = jnp.where(is_static, owns * w, factor)
                    total += field * factor
                sums.append(jnp.sum(total, 0, keepdims=True))
            at = pl.ds(aligned(lv * rows + b * step + i * GROUP, GROUP), GROUP)
            part[at, :] = jnp.concatenate(sums, 0)
            return carry

        lax.fori_loop(0, step // GROUP, eight_rows, 0)
        at = pl.ds(aligned(lv * rows + b * step, GROUP), step)
        remote(part.at[at, :], peer.at[at, :], ms.at[c], mr.at[c], mem_peer)

    def finish(c):
        at = pl.ds(aligned(c * step, GROUP), step)
        wait(peer.at[at, :], mr.at[c])
        out[at, :] = part[at, :] + peer[at, :]

    lag_back = blocks + 1
    lag_grid = lag_back + 2
    lag_sum = lag_grid + 2
    lag_end = lag_sum + 1

    def one_step(t, carry):
        @pl.when(t + AHEAD < chunks)
        def _():
            send_strips(t + AHEAD)

        @pl.when(t < chunks)
        def _():
            forward(t)

        @pl.when((lax.rem(t, blocks) == 1 % blocks) & (t > blocks) & (t < lag_back + chunks))
        def _():
            spectral(lax.div(t - 1, blocks) - 1)

        @pl.when((t >= lag_back) & (t < lag_back + chunks))
        def _():
            backward(t - lag_back)

        @pl.when((t >= lag_grid) & (t < lag_grid + chunks))
        def _():
            to_grid(t - lag_grid)

        @pl.when((t >= lag_sum) & (t < lag_sum + chunks))
        def _():
            gather_sum(t - lag_sum)

        @pl.when((t >= lag_end) & (t < lag_end + chunks))
        def _():
            finish(t - lag_end)

        return carry

    lax.fori_loop(0, chunks + lag_end, one_step, 0)

    def drain(c, carry):
        lv, b = split(c)
        wait(xin.at[lv, : n_lon - 1, :, cells(b)], xs.at[c])
        wait(wst.at[lv, : n_lat - 1, band(b), :], zs.at[c])
        wait(zin.at[lv, : n_lat - 1, band(b), :], bs.at[c])
        wait(xin.at[lv, : n_lon - 1, :, cells(b)], gs.at[c])
        wait(part.at[pl.ds(aligned(c * step, GROUP), step), :], ms.at[c])
        return carry

    lax.fori_loop(0, chunks, drain, 0)


def in_one_kernel(
    control, perturbs, static_input, lat_basis, local_spectrum, static_spectrum, static_weight
):
    mem_dev, levels = control.shape[:2]
    cells = control.shape[-1]
    n_lat, n_lon = lax.axis_size("lat"), lax.axis_size("lon")
    rows = NLAT // n_lat
    cols = cells // rows
    step = STEP_ROWS
    klat = lat_basis.shape[1]
    chunks = levels * rows // step
    plain = lambda a: jnp.moveaxis(a.reshape(mem_dev, levels, cells), 0, 1)
    ctrl, pert = plain(control), plain(perturbs)
    tail = mem_dev + 1 - GROUP
    ctrl_last = jnp.concatenate([ctrl[:, tail:], static_input.reshape(levels, 1, cells)], 1)
    pert_last = jnp.pad(pert[:, tail:], ((0, 0), (0, 1), (0, 0)))

    def pair_of(even, odd):
        return jnp.concatenate(
            [even[:, :LANES], odd[:, :LANES], even[:, LANES:], odd[:, LANES:]], 1
        )

    own = jnp.where(lax.axis_index("lon") == n_lon - 1, static_spectrum, local_spectrum)
    spec = jnp.stack([pair_of(local_spectrum, local_spectrum), pair_of(local_spectrum, own)])
    table = jnp.asarray(packed_table(n_lat))
    sizes = (levels, n_lat, n_lon, rows, cols, step)
    pair = 3 * LANES
    packed = GROUP // 2 * pair
    sems = lambda n: pltpu.SemaphoreType.DMA((n,))
    hbm = pl.BlockSpec(memory_space=pl.ANY)
    result = pl.pallas_call(
        functools.partial(kernel, sizes),
        out_shape=jax.ShapeDtypeStruct((levels * rows, cols), F32),
        in_specs=[hbm] * 8 + [pl.BlockSpec(memory_space=pltpu.SMEM)],
        out_specs=pl.BlockSpec(memory_space=pltpu.VMEM),
        scratch_shapes=[
            pltpu.VMEM((levels, n_lon, GROUP, cells), BF16),
            pltpu.VMEM((levels, n_lat, rows, packed), BF16),
            pltpu.VMEM((levels, n_lat, rows, packed), BF16),
            pltpu.VMEM((levels, n_lat, rows, packed), BF16),
            pltpu.VMEM((levels, n_lon, GROUP, cells), BF16),
            pltpu.VMEM(table.shape, BF16),
            pltpu.VMEM((n_lat, rows, klat), BF16),
            pltpu.VMEM((klat, NLAT), BF16),
            pltpu.VMEM(spec.shape, F32),
            pltpu.VMEM((klat, packed), BF16),
            pltpu.VMEM((step * GROUP, NLON), BF16),
            pltpu.VMEM((table.shape[1] // LANES, step * GROUP, LANES), F32),
            pltpu.VMEM((step * GROUP, table.shape[1]), BF16),
            pltpu.VMEM((2, cols // LANES, step * GROUP, LANES), F32),
            pltpu.VMEM((2, n_lon, GROUP, step * cols), BF16),
            pltpu.VMEM((levels * rows, cols), F32),
            pltpu.VMEM((levels * rows, cols), F32),
            sems(4),
            *[sems(chunks)] * 10,
            sems(2),
        ],
        compiler_params=pltpu.CompilerParams(
            collective_id=0, has_side_effects=True, vmem_limit_bytes=67043328
        ),
        name="covariance",
    )(
        ctrl, ctrl_last, pert, pert_last, table,
        lat_basis.reshape(n_lat, rows, klat), lat_basis.T, spec, static_weight,
    )
    return result.reshape(levels, 1, 1, cells)


def mul(spec, a, b):
    return jnp.einsum(spec, a, b, preferred_element_type=jnp.float32)


def by_waves(
    control, perturbs, static_input, lat_basis, local_spectrum, static_spectrum, static_weight
):
    mem_dev, levels = (control.shape[0], control.shape[1])
    cell_count = control.shape[-1]
    lat_rows = NLAT // lax.axis_size("lat")
    lon_cols = cell_count // lat_rows
    fields = jnp.concatenate([control, static_input[None]], 0).reshape(-1, lat_rows, lon_cols)
    per_lon = fields.shape[0] // lax.axis_size("lon")
    field_index = lax.axis_index("lon") * per_lon + jnp.arange(per_lon, dtype=jnp.int32)
    is_static = field_index >= mem_dev * levels
    first_mem = (lax.axis_index("mem") == 0).astype(jnp.float32)
    zonal = jnp.asarray(zonal_table())
    strips = lax.all_to_all(fields, "lon", split_axis=0, concat_axis=2, tiled=True)
    waves = mul("bxn,nk->kbx", strips, zonal).astype(jnp.bfloat16)
    merid = lax.all_to_all(waves, "lat", split_axis=0, concat_axis=2, tiled=True)
    coef = mul("kby,yj->kbj", merid, lat_basis)
    spectrum = jnp.where(
        is_static[None, :, None], static_spectrum.T[:, None, :], local_spectrum.T[:, None, :]
    )
    scaled = (coef * spectrum).astype(jnp.bfloat16)
    back = mul("kbj,yj->kby", scaled, lat_basis).astype(jnp.bfloat16)
    zonal_rows = lax.all_to_all(back, "lat", split_axis=2, concat_axis=0, tiled=True)
    grid = mul("kbx,nk->bxn", zonal_rows, zonal).astype(jnp.bfloat16)
    pert_fields = perturbs.reshape(mem_dev, levels, lat_rows, lon_cols)
    weight = static_weight[:, None, None]
    filtered = lax.all_to_all(grid, "lon", split_axis=2, concat_axis=0, tiled=True).reshape(
        mem_dev + 1, levels, lat_rows, lon_cols
    )
    ensemble = mul("mlxn,mlxn->lxn", pert_fields, filtered[:mem_dev])
    static_part = filtered[mem_dev].astype(jnp.float32)
    own = first_mem * weight * static_part + (1.0 - weight) * ensemble
    total = lax.psum(own, "mem")
    return total.reshape(levels, 1, 1, cell_count)


def fits(control):
    n_mem, n_lat, n_lon = (lax.axis_size(a) for a in ("mem", "lat", "lon"))
    rows = NLAT // n_lat
    cols = control.shape[-1] // rows
    return (
        n_mem == 2
        and control.shape[0] + 1 == GROUP * n_lon
        and KLON // n_lat == LANES + HALF
        and n_lat & (n_lat - 1) == 0
        and n_lon & (n_lon - 1) == 0
        and rows % STEP_ROWS == 0
        and cols % LANES == 0
        and rows // STEP_ROWS > 1
    )


def solution(mesh):
    def shards(control, *rest):
        body = in_one_kernel if fits(control) else by_waves
        return body(control, *rest)

    return jax.shard_map(
        shards,
        mesh=mesh,
        in_specs=(
            P("mem", None, "lat", "lon", None),
            P("mem", None, "lat", "lon", None),
            P(None, "lat", "lon", None),
            P(),
            P(None, "lat"),
            P(None, "lat"),
            P(),
        ),
        out_specs=P(None, "lat", "lon", None),
        check_vma=False,
    )
```

```python
import functools

import jax
import jax.numpy as jnp
import numpy as np
from jax import lax
from jax.experimental import pallas as pl
from jax.experimental.pallas import tpu as pltpu
from jax.sharding import PartitionSpec as P

NLON = 1536
NLAT = 768
KLON = 768
LANES = 128
HALF = 64
GROUP = 8
STEP_ROWS = 16
AHEAD = 4
MESH = pl.DeviceIdType.MESH
F32, BF16 = jnp.float32, jnp.bfloat16


def zonal_table():
    half = KLON // 2
    column = np.arange(KLON)
    wave = np.where(column < half, column, column - half + 1)
    angle = 2.0 * np.pi / NLON * (np.arange(NLON)[:, None] * wave[None, :] % NLON)
    values = np.where(column[None, :] < half, np.cos(angle), np.sin(angle))
    return (np.sqrt(2.0 / NLON) * values).astype(jnp.bfloat16)


def packed_table(n_lat):
    blocks = zonal_table().reshape(NLON, n_lat, KLON // n_lat)
    main = blocks[:, :, :LANES].reshape(NLON, -1)
    rest = blocks[:, :, LANES:]
    swapped = rest.reshape(NLON, n_lat // 2, 2, HALF)[:, :, ::-1]
    return np.concatenate([main, rest.reshape(NLON, -1), swapped.reshape(NLON, -1)], 1)


def aligned(start, to):
    return pl.multiple_of(start, to)


def kernel(
    sizes,
    ctrl, pert, static_in, table_in, merid_in, local_in, global_in, weight,
    out,
    xin, wst, zin, bin_, gin, table, merid, merid_t, spec,
    scaled, rows_in, waves, rows_out, grid, cbuf, pbuf, static, local_t, global_t, part, peer,
    csem, xs, xr, zs, zr, bs, br, gs, gr, ms, mr, cs, ps,
):
    levels, n_lat, n_lon, rows, cols, step = sizes
    blocks = rows // step
    chunks = levels * blocks
    width = step * cols
    pair = 3 * LANES
    pairs = GROUP // 2
    rest_a = n_lat * LANES
    rest_b = rest_a + n_lat * HALF
    my_mem, my_lat, my_lon = lax.axis_index("mem"), lax.axis_index("lat"), lax.axis_index("lon")
    lon_order = [2, 3, 1] if n_lon == 4 else list(range(1, n_lon))
    lat_order = [2, 3, 1] if n_lat == 4 else list(range(1, n_lat))

    def at_lon(lon):
        return (my_mem, my_lat, lon)

    def at_lat(lat):
        return (my_mem, lat, my_lon)

    def split(c):
        return lax.div(c, blocks), lax.rem(c, blocks)

    def cells(b):
        return pl.ds(aligned(b * width, LANES), width)

    def band(b):
        return pl.ds(aligned(b * step, 16), step)

    def remote(src, dst, send, recv, device):
        pltpu.make_async_remote_copy(
            src_ref=src, dst_ref=dst, send_sem=send, recv_sem=recv,
            device_id=device, device_id_type=MESH,
        ).start()

    def wait(ref, sem):
        pltpu.make_async_copy(ref, ref, sem).wait()

    tail = (n_lon - 1) * GROUP
    consts = [
        (static_in, static), (merid_in, merid), (local_in, local_t), (global_in, global_t),
        (table_in, table),
    ]
    for i, (src, dst) in enumerate(consts):
        pltpu.make_async_copy(src, dst, csem.at[i]).start()

    barrier = pltpu.get_barrier_semaphore()
    for s in range(1, n_lon):
        pl.semaphore_signal(barrier, 1, device_id=at_lon(my_lon ^ s), device_id_type=MESH)
    for s in range(1, n_lat):
        pl.semaphore_signal(barrier, 1, device_id=at_lat(my_lat ^ s), device_id_type=MESH)
    mem_peer = (1 - my_mem, my_lat, my_lon)
    pl.semaphore_signal(barrier, 1, device_id=mem_peer, device_id_type=MESH)
    pl.semaphore_wait(barrier, n_lon + n_lat - 1)

    def load_members(src, buf, sem, c):
        lv, b = split(c)
        slot = lax.rem(c, 2)
        return pltpu.make_async_copy(src.at[lv, :, cells(b)], buf.at[slot], sem.at[slot])

    def send_strips(c):
        lv, b = split(c)
        dst = xin.at[lv, my_lon, :, cells(b)]
        stage = gin.at[lv, my_lon, :, cells(b)]

        def strip(lon):
            return ctrl.at[lv, pl.ds(aligned(lon * GROUP, GROUP), GROUP), cells(b)]

        def send(src, lon):
            remote(src, dst, xs.at[c], xr.at[c], at_lon(lon))

        for s in lon_order:
            lon = my_lon ^ s

            @pl.when(lon < n_lon - 1)
            def _(lon=lon):
                send(strip(lon), lon)

        load_members(ctrl, cbuf, cs, c).wait()

        @pl.when(c + 1 < chunks)
        def _():
            load_members(ctrl, cbuf, cs, c + 1).start()

        def two_rows(i, carry):
            at = pl.ds(aligned(i * (2 * cols), LANES), 2 * cols)
            all_at = pl.ds(aligned(b * width + i * (2 * cols), LANES), 2 * cols)
            x = cbuf[lax.rem(c, 2), tail:, at].astype(F32)
            v = static[:, all_at].astype(F32)
            row = v[levels - 1 : levels]
            for k in range(levels - 1):
                row = jnp.where(lv == k, v[k : k + 1], row)
            gin[lv, my_lon, :, all_at] = jnp.concatenate([x, row], 0).astype(BF16)
            return carry

        lax.fori_loop(0, step // 2, two_rows, 0)

        @pl.when(my_lon < n_lon - 1)
        def _():
            send(stage, n_lon - 1)
            pltpu.make_async_copy(strip(my_lon), dst, xr.at[c]).start()

        @pl.when(my_lon == n_lon - 1)
        def _():
            pltpu.make_async_copy(stage, dst, xr.at[c]).start()

    load_members(ctrl, cbuf, cs, 0).start()
    load_members(pert, pbuf, ps, 0).start()
    pltpu.make_async_copy(static_in, static, csem.at[0]).wait()
    for c in range(min(AHEAD, chunks)):
        send_strips(c)
    for i, (src, dst) in enumerate(consts[1:]):
        pltpu.make_async_copy(src, dst, csem.at[i + 1]).wait()
    for d in range(n_lat):
        merid_t[d] = merid[d].astype(F32).T.astype(BF16)
    shared = jnp.where(my_lon == n_lon - 1, global_t[...], local_t[...])
    for kind, (even, odd) in enumerate([(local_t[...], local_t[...]), (local_t[...], shared)]):
        both = jnp.concatenate([even[:LANES], odd[:LANES], even[LANES:], odd[LANES:]], 0)
        spec[kind] = both.T

    low = lax.broadcasted_iota(jnp.int32, (step, LANES), 1) < HALF
    low_16 = low.astype(F32).astype(BF16)
    high_16 = (1.0 - low.astype(F32)).astype(BF16)

    def forward(c):
        lv, b = split(c)
        wait(xin.at[lv, :, :, cells(b)], xr.at[c])

        def two_rows(i, carry):
            for e in range(n_lon):
                at = pl.ds(aligned(b * width + i * (2 * cols), LANES), 2 * cols)
                x = xin[lv, e, :, at].astype(F32)
                x = jnp.concatenate([x[:, :cols], x[:, cols:]], 0).astype(BF16)
                rows_in[pl.ds(aligned(i * 16, 16), 16), e * cols : (e + 1) * cols] = x
            return carry

        lax.fori_loop(0, step // 2, two_rows, 0)
        for k in range(0, waves.shape[0], 2):
            at = slice(k * LANES, (k + 2) * LANES)
            pair_k = jnp.dot(rows_in[...], table[:, at], preferred_element_type=F32)
            waves[k] = pair_k[:, :LANES]
            waves[k + 1] = pair_k[:, LANES:]
        for p in range(pairs):
            for d in range(n_lat):
                main = d
                in_a = rest_a // LANES + d // 2
                in_b = rest_b // LANES + d // 2
                first, second = (in_a, in_b) if d % 2 == 0 else (in_b, in_a)
                even, odd = pl.ds(2 * p, step, GROUP), pl.ds(2 * p + 1, step, GROUP)
                last = jnp.where(low, waves[first, even, :], waves[second, odd, :])
                at = p * pair
                wst[lv, d, band(b), at : at + LANES] = waves[main, even, :].astype(BF16)
                wst[lv, d, band(b), at + LANES : at + 2 * LANES] = waves[main, odd, :].astype(BF16)
                wst[lv, d, band(b), at + 2 * LANES : at + pair] = last.astype(BF16)
        dst = zin.at[lv, my_lat, band(b), :]
        for s in lat_order:
            lat = my_lat ^ s
            remote(wst.at[lv, lat, band(b), :], dst, zs.at[c], zr.at[c], at_lat(lat))
        pltpu.make_async_copy(wst.at[lv, my_lat, band(b), :], dst, zr.at[c]).start()

    def spectral(lv):
        def arrived(b, carry):
            wait(zin.at[lv, :, band(b), :], zr.at[lv * blocks + b])
            return carry

        lax.fori_loop(0, blocks, arrived, 0)
        for p in range(pairs):
            at = slice(p * pair, (p + 1) * pair)
            coef = sum(
                jnp.dot(merid_t[d], zin[lv, d, :, at], preferred_element_type=F32)
                for d in range(n_lat)
            )
            kind = 1 if p == pairs - 1 else 0
            scaled[:, at] = (coef * spec[kind]).astype(BF16)

    def backward(c):
        lv, b = split(c)
        lhs = jnp.concatenate([merid[d, band(b), :] for d in range(n_lat)], 0)
        for p in range(pairs):
            at = slice(p * pair, (p + 1) * pair)
            back = jnp.dot(lhs, scaled[:, at], preferred_element_type=F32).astype(BF16)
            for d in range(n_lat):
                zin[lv, d, band(b), at] = back[d * step : (d + 1) * step]
        dst = bin_.at[lv, my_lat, band(b), :]
        for s in lat_order:
            lat = my_lat ^ s
            remote(zin.at[lv, lat, band(b), :], dst, bs.at[c], br.at[c], at_lat(lat))
        pltpu.make_async_copy(zin.at[lv, my_lat, band(b), :], dst, br.at[c]).start()

    def to_grid(c):
        lv, b = split(c)
        wait(bin_.at[lv, :, band(b), :], br.at[c])
        for p in range(pairs):
            even = slice(2 * p * step, (2 * p + 1) * step)
            odd = slice((2 * p + 1) * step, (2 * p + 2) * step)
            at = p * pair
            for s in range(n_lat):
                main = slice(s * LANES, (s + 1) * LANES)
                in_a = slice(rest_a + s // 2 * LANES, rest_a + (s // 2 + 1) * LANES)
                in_b = slice(rest_b + s // 2 * LANES, rest_b + (s // 2 + 1) * LANES)
                first, second = (in_a, in_b) if s % 2 == 0 else (in_b, in_a)
                rest = bin_[lv, s, band(b), at + 2 * LANES : at + pair]
                rows_out[even, main] = bin_[lv, s, band(b), at : at + LANES]
                rows_out[odd, main] = bin_[lv, s, band(b), at + LANES : at + 2 * LANES]
                rows_out[even, first] = rest * low_16
                rows_out[odd, second] = rest * high_16
        for e in range(n_lon):
            part_e = lax.dot_general(
                rows_out[...], table[e * cols : (e + 1) * cols, :],
                (((1,), (1,)), ((), ())), preferred_element_type=F32,
            )
            for m in range(GROUP):
                for j in range(cols // LANES):
                    tile = part_e[m * step : (m + 1) * step, j * LANES : (j + 1) * LANES]
                    grid[e % 2, j, pl.ds(m, step, GROUP), :] = tile

            def two_rows(i, carry):
                x = [
                    grid[e % 2, j, pl.ds(aligned(i * 16 + h, GROUP), GROUP), :]
                    for h in (0, GROUP)
                    for j in range(cols // LANES)
                ]
                x = jnp.concatenate(x, 1).astype(BF16)
                at = pl.ds(aligned(b * width + i * (2 * cols), LANES), 2 * cols)
                xin[lv, e, :, at] = x
                return carry

            lax.fori_loop(0, step // 2, two_rows, 0)
        dst = gin.at[lv, my_lon, :, cells(b)]
        wait(xin.at[lv, : n_lon - 1, :, cells(b)], xs.at[c])
        for s in lon_order:
            lon = my_lon ^ s
            remote(xin.at[lv, lon, :, cells(b)], dst, gs.at[c], gr.at[c], at_lon(lon))
        pltpu.make_async_copy(xin.at[lv, my_lon, :, cells(b)], dst, gr.at[c]).start()

    owns = jnp.where(my_mem == 0, 1.0, 0.0).astype(F32)

    def gather_sum(c):
        lv, b = split(c)
        slot = lax.rem(c, 2)
        load_members(pert, pbuf, ps, c).wait()

        @pl.when(c + 1 < chunks)
        def _():
            load_members(pert, pbuf, ps, c + 1).start()

        wait(gin.at[lv, :, :, cells(b)], gr.at[c])
        w = weight[lv]

        def eight_rows(i, carry):
            sums = []
            for y in range(GROUP):
                off = aligned(i * (GROUP * cols) + y * cols, LANES)
                total = jnp.zeros((GROUP, cols), F32)
                here = pl.ds(off, cols)
                there = pl.ds(aligned(b * width + off, LANES), cols)
                for e in range(n_lon - 1):
                    factor = pbuf[slot, e * GROUP : (e + 1) * GROUP, here].astype(F32)
                    total += gin[lv, e, :, there].astype(F32) * factor
                field = gin[lv, n_lon - 1, :, there].astype(F32)
                last = field[: GROUP - 1] * pbuf[slot, tail:, here].astype(F32)
                total = (1.0 - w) * (jnp.sum(total, 0, keepdims=True) + jnp.sum(last, 0, keepdims=True))
                total += owns * w * field[GROUP - 1 :]
                sums.append(total)
            at = pl.ds(aligned(lv * rows + b * step + i * GROUP, GROUP), GROUP)
            part[at, :] = jnp.concatenate(sums, 0)
            return carry

        lax.fori_loop(0, step // GROUP, eight_rows, 0)
        at = pl.ds(aligned(lv * rows + b * step, GROUP), step)
        remote(part.at[at, :], peer.at[at, :], ms.at[c], mr.at[c], mem_peer)

    def finish(c):
        at = pl.ds(aligned(c * step, GROUP), step)
        wait(peer.at[at, :], mr.at[c])
        both = part[at, :] + peer[at, :]
        lv, b = split(c)
        for y in range(step):
            there = pl.ds(aligned(b * width + y * cols, LANES), cols)
            out[pl.ds(lv, 1), there] = both[y : y + 1]

    lag_back = blocks + 1
    lag_grid = lag_back + 2
    lag_sum = lag_grid + 2
    lag_end = lag_sum + 1

    def one_step(t, carry):
        @pl.when(t + AHEAD < chunks)
        def _():
            send_strips(t + AHEAD)

        @pl.when(t < chunks)
        def _():
            forward(t)

        @pl.when((lax.rem(t, blocks) == 1 % blocks) & (t > blocks) & (t < lag_back + chunks))
        def _():
            spectral(lax.div(t - 1, blocks) - 1)

        @pl.when((t >= lag_back) & (t < lag_back + chunks))
        def _():
            backward(t - lag_back)

        @pl.when((t >= lag_grid) & (t < lag_grid + chunks))
        def _():
            to_grid(t - lag_grid)

        @pl.when((t >= lag_sum) & (t < lag_sum + chunks))
        def _():
            gather_sum(t - lag_sum)

        @pl.when((t >= lag_end) & (t < lag_end + chunks))
        def _():
            finish(t - lag_end)

        return carry

    lax.fori_loop(0, chunks + lag_end, one_step, 0)

    def drain(c, carry):
        lv, b = split(c)
        wait(wst.at[lv, : n_lat - 1, band(b), :], zs.at[c])
        wait(zin.at[lv, : n_lat - 1, band(b), :], bs.at[c])
        wait(xin.at[lv, : n_lon - 1, :, cells(b)], gs.at[c])
        wait(part.at[pl.ds(aligned(c * step, GROUP), step), :], ms.at[c])
        return carry

    lax.fori_loop(0, chunks, drain, 0)


def in_one_kernel(
    control, perturbs, static_input, lat_basis, local_spectrum, static_spectrum, static_weight
):
    mem_dev, levels = control.shape[:2]
    cells = control.shape[-1]
    n_lat, n_lon = lax.axis_size("lat"), lax.axis_size("lon")
    rows = NLAT // n_lat
    cols = cells // rows
    step = STEP_ROWS
    klat = lat_basis.shape[1]
    chunks = levels * rows // step
    plain = lambda a: jnp.moveaxis(a.reshape(mem_dev, levels, cells), 0, 1)
    ctrl, pert = plain(control), plain(perturbs)
    table = jnp.asarray(packed_table(n_lat))
    sizes = (levels, n_lat, n_lon, rows, cols, step)
    pair = 3 * LANES
    packed = GROUP // 2 * pair
    sems = lambda n: pltpu.SemaphoreType.DMA((n,))
    hbm = pl.BlockSpec(memory_space=pl.ANY)
    result = pl.pallas_call(
        functools.partial(kernel, sizes),
        out_shape=jax.ShapeDtypeStruct((levels, cells), F32),
        in_specs=[hbm] * 7 + [pl.BlockSpec(memory_space=pltpu.SMEM)],
        out_specs=pl.BlockSpec(memory_space=pltpu.VMEM),
        scratch_shapes=[
            pltpu.VMEM((levels, n_lon, GROUP, cells), BF16),
            pltpu.VMEM((levels, n_lat, rows, packed), BF16),
            pltpu.VMEM((levels, n_lat, rows, packed), BF16),
            pltpu.VMEM((levels, n_lat, rows, packed), BF16),
            pltpu.VMEM((levels, n_lon, GROUP, cells), BF16),
            pltpu.VMEM(table.shape, BF16),
            pltpu.VMEM((n_lat, rows, klat), BF16),
            pltpu.VMEM((n_lat, klat, rows), BF16),
            pltpu.VMEM((2, klat, pair), F32),
            pltpu.VMEM((klat, packed), BF16),
            pltpu.VMEM((step * GROUP, NLON), BF16),
            pltpu.VMEM((table.shape[1] // LANES, step * GROUP, LANES), F32),
            pltpu.VMEM((step * GROUP, table.shape[1]), BF16),
            pltpu.VMEM((2, cols // LANES, step * GROUP, LANES), F32),
            pltpu.VMEM((2, mem_dev, step * cols), BF16),
            pltpu.VMEM((2, mem_dev, step * cols), BF16),
            pltpu.VMEM((levels, cells), BF16),
            pltpu.VMEM(local_spectrum.shape[::-1], F32),
            pltpu.VMEM(local_spectrum.shape[::-1], F32),
            pltpu.VMEM((levels * rows, cols), F32),
            pltpu.VMEM((levels * rows, cols), F32),
            sems(5),
            *[sems(chunks)] * 10,
            sems(2),
            sems(2),
        ],
        compiler_params=pltpu.CompilerParams(
            collective_id=0, has_side_effects=True, vmem_limit_bytes=67043328
        ),
        name="covariance",
    )(
        ctrl, pert, static_input.reshape(levels, cells), table,
        lat_basis.reshape(n_lat, rows, klat), local_spectrum.T, static_spectrum.T, static_weight,
    )
    return result.reshape(levels, 1, 1, cells)


def mul(spec, a, b):
    return jnp.einsum(spec, a, b, preferred_element_type=jnp.float32)


def by_waves(
    control, perturbs, static_input, lat_basis, local_spectrum, static_spectrum, static_weight
):
    mem_dev, levels = (control.shape[0], control.shape[1])
    cell_count = control.shape[-1]
    lat_rows = NLAT // lax.axis_size("lat")
    lon_cols = cell_count // lat_rows
    fields = jnp.concatenate([control, static_input[None]], 0).reshape(-1, lat_rows, lon_cols)
    per_lon = fields.shape[0] // lax.axis_size("lon")
    field_index = lax.axis_index("lon") * per_lon + jnp.arange(per_lon, dtype=jnp.int32)
    is_static = field_index >= mem_dev * levels
    first_mem = (lax.axis_index("mem") == 0).astype(jnp.float32)
    zonal = jnp.asarray(zonal_table())
    strips = lax.all_to_all(fields, "lon", split_axis=0, concat_axis=2, tiled=True)
    waves = mul("bxn,nk->kbx", strips, zonal).astype(jnp.bfloat16)
    merid = lax.all_to_all(waves, "lat", split_axis=0, concat_axis=2, tiled=True)
    coef = mul("kby,yj->kbj", merid, lat_basis)
    spectrum = jnp.where(
        is_static[None, :, None], static_spectrum.T[:, None, :], local_spectrum.T[:, None, :]
    )
    scaled = (coef * spectrum).astype(jnp.bfloat16)
    back = mul("kbj,yj->kby", scaled, lat_basis).astype(jnp.bfloat16)
    zonal_rows = lax.all_to_all(back, "lat", split_axis=2, concat_axis=0, tiled=True)
    grid = mul("kbx,nk->bxn", zonal_rows, zonal).astype(jnp.bfloat16)
    pert_fields = perturbs.reshape(mem_dev, levels, lat_rows, lon_cols)
    weight = static_weight[:, None, None]
    filtered = lax.all_to_all(grid, "lon", split_axis=2, concat_axis=0, tiled=True).reshape(
        mem_dev + 1, levels, lat_rows, lon_cols
    )
    ensemble = mul("mlxn,mlxn->lxn", pert_fields, filtered[:mem_dev])
    static_part = filtered[mem_dev].astype(jnp.float32)
    own = first_mem * weight * static_part + (1.0 - weight) * ensemble
    total = lax.psum(own, "mem")
    return total.reshape(levels, 1, 1, cell_count)


def fits(control):
    n_mem, n_lat, n_lon = (lax.axis_size(a) for a in ("mem", "lat", "lon"))
    rows = NLAT // n_lat
    cols = control.shape[-1] // rows
    return (
        n_mem == 2
        and control.shape[0] + 1 == GROUP * n_lon
        and KLON // n_lat == LANES + HALF
        and n_lat & (n_lat - 1) == 0
        and n_lon & (n_lon - 1) == 0
        and rows % STEP_ROWS == 0
        and cols % LANES == 0
        and rows // STEP_ROWS > 1
    )


def solution(mesh):
    def shards(control, *rest):
        body = in_one_kernel if fits(control) else by_waves
        return body(control, *rest)

    return jax.shard_map(
        shards,
        mesh=mesh,
        in_specs=(
            P("mem", None, "lat", "lon", None),
            P("mem", None, "lat", "lon", None),
            P(None, "lat", "lon", None),
            P(),
            P(None, "lat"),
            P(None, "lat"),
            P(),
        ),
        out_specs=P(None, "lat", "lon", None),
        check_vma=False,
    )
```

```python
import functools

import jax
import jax.numpy as jnp
import numpy as np
from jax import lax
from jax.experimental import pallas as pl
from jax.experimental.pallas import tpu as pltpu
from jax.sharding import PartitionSpec as P

NLON = 1536
NLAT = 768
KLON = 768
LANES = 128
HALF = 64
GROUP = 8
STEP_ROWS = 16
AHEAD = 4
MESH = pl.DeviceIdType.MESH
F32, BF16 = jnp.float32, jnp.bfloat16


def zonal_table():
    half = KLON // 2
    column = np.arange(KLON)
    wave = np.where(column < half, column, column - half + 1)
    angle = 2.0 * np.pi / NLON * (np.arange(NLON)[:, None] * wave[None, :] % NLON)
    values = np.where(column[None, :] < half, np.cos(angle), np.sin(angle))
    return (np.sqrt(2.0 / NLON) * values).astype(jnp.bfloat16)


def packed_table(n_lat):
    blocks = zonal_table().reshape(NLON, n_lat, KLON // n_lat)
    main = blocks[:, :, :LANES].reshape(NLON, -1)
    rest = blocks[:, :, LANES:]
    swapped = rest.reshape(NLON, n_lat // 2, 2, HALF)[:, :, ::-1]
    return np.concatenate([main, rest.reshape(NLON, -1), swapped.reshape(NLON, -1)], 1)


def aligned(start, to):
    return pl.multiple_of(start, to)


def kernel(
    sizes,
    ctrl, pert, static_in, table_in, merid_in, local_in, global_in, weight,
    out,
    xin, wst, zin, bin_, gin, table, merid, merid_t, spec,
    scaled, rows_in, waves, rows_out, grid, cbuf, pbuf, static, local_t, global_t, part, peer,
    csem, xs, xr, zs, zr, bs, br, gs, gr, ms, mr, cs, ps,
):
    levels, n_lat, n_lon, rows, cols, step = sizes
    blocks = rows // step
    chunks = levels * blocks
    width = step * cols
    pair = 3 * LANES
    pairs = GROUP // 2
    rest_a = n_lat * LANES
    rest_b = rest_a + n_lat * HALF
    my_mem, my_lat, my_lon = lax.axis_index("mem"), lax.axis_index("lat"), lax.axis_index("lon")
    lon_order = [2, 3, 1] if n_lon == 4 else list(range(1, n_lon))
    lat_order = [2, 3, 1] if n_lat == 4 else list(range(1, n_lat))

    def at_lon(lon):
        return (my_mem, my_lat, lon)

    def at_lat(lat):
        return (my_mem, lat, my_lon)

    def split(c):
        return lax.div(c, blocks), lax.rem(c, blocks)

    def cells(b):
        return pl.ds(aligned(b * width, LANES), width)

    def band(b):
        return pl.ds(aligned(b * step, 16), step)

    def remote(src, dst, send, recv, device):
        pltpu.make_async_remote_copy(
            src_ref=src, dst_ref=dst, send_sem=send, recv_sem=recv,
            device_id=device, device_id_type=MESH,
        ).start()

    def wait(ref, sem):
        pltpu.make_async_copy(ref, ref, sem).wait()

    tail = (n_lon - 1) * GROUP
    consts = [
        (static_in, static), (merid_in, merid), (local_in, local_t), (global_in, global_t),
        (table_in, table),
    ]
    for i, (src, dst) in enumerate(consts):
        pltpu.make_async_copy(src, dst, csem.at[i]).start()

    barrier = pltpu.get_barrier_semaphore()
    for s in range(1, n_lon):
        pl.semaphore_signal(barrier, 1, device_id=at_lon(my_lon ^ s), device_id_type=MESH)
    for s in range(1, n_lat):
        pl.semaphore_signal(barrier, 1, device_id=at_lat(my_lat ^ s), device_id_type=MESH)
    mem_peer = (1 - my_mem, my_lat, my_lon)
    pl.semaphore_signal(barrier, 1, device_id=mem_peer, device_id_type=MESH)
    pl.semaphore_wait(barrier, n_lon + n_lat - 1)

    def load_members(src, buf, sem, c):
        lv, b = split(c)
        slot = lax.rem(c, 2)
        return pltpu.make_async_copy(src.at[lv, :, cells(b)], buf.at[slot], sem.at[slot])

    def send_strips(c):
        lv, b = split(c)
        dst = xin.at[lv, my_lon, :, cells(b)]
        stage = gin.at[lv, my_lon, :, cells(b)]

        def strip(lon):
            return ctrl.at[lv, pl.ds(aligned(lon * GROUP, GROUP), GROUP), cells(b)]

        def send(src, lon):
            remote(src, dst, xs.at[c], xr.at[c], at_lon(lon))

        for s in lon_order:
            lon = my_lon ^ s

            @pl.when(lon < n_lon - 1)
            def _(lon=lon):
                send(strip(lon), lon)

        load_members(ctrl, cbuf, cs, c).wait()

        @pl.when(c + 1 < chunks)
        def _():
            load_members(ctrl, cbuf, cs, c + 1).start()

        def two_rows(i, carry):
            at = pl.ds(aligned(i * (2 * cols), LANES), 2 * cols)
            all_at = pl.ds(aligned(b * width + i * (2 * cols), LANES), 2 * cols)
            x = cbuf[lax.rem(c, 2), tail:, at].astype(F32)
            v = static[:, all_at].astype(F32)
            row = v[levels - 1 : levels]
            for k in range(levels - 1):
                row = jnp.where(lv == k, v[k : k + 1], row)
            gin[lv, my_lon, :, all_at] = jnp.concatenate([x, row], 0).astype(BF16)
            return carry

        lax.fori_loop(0, step // 2, two_rows, 0)

        @pl.when(my_lon < n_lon - 1)
        def _():
            send(stage, n_lon - 1)
            pltpu.make_async_copy(strip(my_lon), dst, xr.at[c]).start()

        @pl.when(my_lon == n_lon - 1)
        def _():
            pltpu.make_async_copy(stage, dst, xr.at[c]).start()

    load_members(ctrl, cbuf, cs, 0).start()
    load_members(pert, pbuf, ps, 0).start()
    pltpu.make_async_copy(static_in, static, csem.at[0]).wait()
    for c in range(min(AHEAD, chunks)):
        send_strips(c)
    for i, (src, dst) in enumerate(consts[1:]):
        pltpu.make_async_copy(src, dst, csem.at[i + 1]).wait()
    for d in range(n_lat):
        merid_t[d] = merid[d].astype(F32).T.astype(BF16)
    shared = jnp.where(my_lon == n_lon - 1, global_t[...], local_t[...])
    for kind, (even, odd) in enumerate([(local_t[...], local_t[...]), (local_t[...], shared)]):
        both = jnp.concatenate([even[:LANES], odd[:LANES], even[LANES:], odd[LANES:]], 0)
        spec[kind] = both.T

    low = lax.broadcasted_iota(jnp.int32, (step, LANES), 1) < HALF
    low_16 = low.astype(F32).astype(BF16)
    high_16 = (1.0 - low.astype(F32)).astype(BF16)

    def forward(c):
        lv, b = split(c)
        wait(xin.at[lv, :, :, cells(b)], xr.at[c])

        for i in range(step // 2):
            for e in range(n_lon):
                at = pl.ds(aligned(b * width + i * (2 * cols), LANES), 2 * cols)
                x = xin[lv, e, :, at].astype(F32)
                x = jnp.concatenate([x[:, :cols], x[:, cols:]], 0).astype(BF16)
                rows_in[i * 16 : (i + 1) * 16, e * cols : (e + 1) * cols] = x
        for k in range(0, waves.shape[0], 2):
            at = slice(k * LANES, (k + 2) * LANES)
            pair_k = jnp.dot(rows_in[...], table[:, at], preferred_element_type=F32)
            waves[k] = pair_k[:, :LANES]
            waves[k + 1] = pair_k[:, LANES:]
        for p in range(pairs):
            for d in range(n_lat):
                main = d
                in_a = rest_a // LANES + d // 2
                in_b = rest_b // LANES + d // 2
                first, second = (in_a, in_b) if d % 2 == 0 else (in_b, in_a)
                even, odd = pl.ds(2 * p, step, GROUP), pl.ds(2 * p + 1, step, GROUP)
                last = jnp.where(low, waves[first, even, :], waves[second, odd, :])
                at = p * pair
                wst[lv, d, band(b), at : at + LANES] = waves[main, even, :].astype(BF16)
                wst[lv, d, band(b), at + LANES : at + 2 * LANES] = waves[main, odd, :].astype(BF16)
                wst[lv, d, band(b), at + 2 * LANES : at + pair] = last.astype(BF16)
        dst = zin.at[lv, my_lat, band(b), :]
        for s in lat_order:
            lat = my_lat ^ s
            remote(wst.at[lv, lat, band(b), :], dst, zs.at[c], zr.at[c], at_lat(lat))
        pltpu.make_async_copy(wst.at[lv, my_lat, band(b), :], dst, zr.at[c]).start()

    def spectral(lv):
        def arrived(b, carry):
            wait(zin.at[lv, :, band(b), :], zr.at[lv * blocks + b])
            return carry

        lax.fori_loop(0, blocks, arrived, 0)
        for p in range(pairs):
            at = slice(p * pair, (p + 1) * pair)
            coef = sum(
                jnp.dot(merid_t[d], zin[lv, d, :, at], preferred_element_type=F32)
                for d in range(n_lat)
            )
            kind = 1 if p == pairs - 1 else 0
            scaled[:, at] = (coef * spec[kind]).astype(BF16)

    def backward(c):
        lv, b = split(c)
        lhs = jnp.concatenate([merid[d, band(b), :] for d in range(n_lat)], 0)
        for p in range(pairs):
            at = slice(p * pair, (p + 1) * pair)
            back = jnp.dot(lhs, scaled[:, at], preferred_element_type=F32).astype(BF16)
            for d in range(n_lat):
                zin[lv, d, band(b), at] = back[d * step : (d + 1) * step]
        dst = bin_.at[lv, my_lat, band(b), :]
        for s in lat_order:
            lat = my_lat ^ s
            remote(zin.at[lv, lat, band(b), :], dst, bs.at[c], br.at[c], at_lat(lat))
        pltpu.make_async_copy(zin.at[lv, my_lat, band(b), :], dst, br.at[c]).start()

    def to_grid(c):
        lv, b = split(c)
        wait(bin_.at[lv, :, band(b), :], br.at[c])
        for p in range(pairs):
            even = slice(2 * p * step, (2 * p + 1) * step)
            odd = slice((2 * p + 1) * step, (2 * p + 2) * step)
            at = p * pair
            for s in range(n_lat):
                main = slice(s * LANES, (s + 1) * LANES)
                in_a = slice(rest_a + s // 2 * LANES, rest_a + (s // 2 + 1) * LANES)
                in_b = slice(rest_b + s // 2 * LANES, rest_b + (s // 2 + 1) * LANES)
                first, second = (in_a, in_b) if s % 2 == 0 else (in_b, in_a)
                rest = bin_[lv, s, band(b), at + 2 * LANES : at + pair]
                rows_out[even, main] = bin_[lv, s, band(b), at : at + LANES]
                rows_out[odd, main] = bin_[lv, s, band(b), at + LANES : at + 2 * LANES]
                rows_out[even, first] = rest * low_16
                rows_out[odd, second] = rest * high_16
        wait(xin.at[lv, : n_lon - 1, :, cells(b)], xs.at[c])
        dst = gin.at[lv, my_lon, :, cells(b)]
        for turn, s in enumerate(lon_order + [0]):
            lon = my_lon ^ s
            strip = table[pl.ds(aligned(lon * cols, LANES), cols), :]
            part_e = lax.dot_general(
                rows_out[...], strip, (((1,), (1,)), ((), ())), preferred_element_type=F32
            )
            for m in range(GROUP):
                for j in range(cols // LANES):
                    tile = part_e[m * step : (m + 1) * step, j * LANES : (j + 1) * LANES]
                    grid[turn % 2, j, pl.ds(m, step, GROUP), :] = tile
            for i in range(step // 2):
                x = [
                    grid[turn % 2, j, i * 16 + h : i * 16 + h + GROUP, :]
                    for h in (0, GROUP)
                    for j in range(cols // LANES)
                ]
                at = pl.ds(aligned(b * width + i * (2 * cols), LANES), 2 * cols)
                xin[lv, lon, :, at] = jnp.concatenate(x, 1).astype(BF16)
            src = xin.at[lv, lon, :, cells(b)]
            if s:
                remote(src, dst, gs.at[c], gr.at[c], at_lon(lon))
            else:
                pltpu.make_async_copy(src, dst, gr.at[c]).start()

    owns = jnp.where(my_mem == 0, 1.0, 0.0).astype(F32)

    def gather_sum(c):
        lv, b = split(c)
        slot = lax.rem(c, 2)
        load_members(pert, pbuf, ps, c).wait()

        @pl.when(c + 1 < chunks)
        def _():
            load_members(pert, pbuf, ps, c + 1).start()

        wait(gin.at[lv, :, :, cells(b)], gr.at[c])
        w = weight[lv]

        def eight_rows(i, carry):
            sums = []
            for y in range(GROUP):
                off = aligned(i * (GROUP * cols) + y * cols, LANES)
                total = jnp.zeros((GROUP, cols), F32)
                here = pl.ds(off, cols)
                there = pl.ds(aligned(b * width + off, LANES), cols)
                for e in range(n_lon - 1):
                    factor = pbuf[slot, e * GROUP : (e + 1) * GROUP, here].astype(F32)
                    total += gin[lv, e, :, there].astype(F32) * factor
                field = gin[lv, n_lon - 1, :, there].astype(F32)
                last = field[: GROUP - 1] * pbuf[slot, tail:, here].astype(F32)
                total = (1.0 - w) * (jnp.sum(total, 0, keepdims=True) + jnp.sum(last, 0, keepdims=True))
                total += owns * w * field[GROUP - 1 :]
                sums.append(total)
            at = pl.ds(aligned(lv * rows + b * step + i * GROUP, GROUP), GROUP)
            part[at, :] = jnp.concatenate(sums, 0)
            return carry

        lax.fori_loop(0, step // GROUP, eight_rows, 0)
        at = pl.ds(aligned(lv * rows + b * step, GROUP), step)
        remote(part.at[at, :], peer.at[at, :], ms.at[c], mr.at[c], mem_peer)

    def finish(c):
        at = pl.ds(aligned(c * step, GROUP), step)
        wait(peer.at[at, :], mr.at[c])
        both = part[at, :] + peer[at, :]
        lv, b = split(c)
        for y in range(step):
            there = pl.ds(aligned(b * width + y * cols, LANES), cols)
            out[lv, :, there] = both[y : y + 1]

    lag_back = blocks + 1
    lag_grid = lag_back + 2
    lag_sum = lag_grid + 2
    lag_end = lag_sum + 1

    def one_step(t, carry):
        @pl.when(t + AHEAD < chunks)
        def _():
            send_strips(t + AHEAD)

        @pl.when(t < chunks)
        def _():
            forward(t)

        @pl.when((lax.rem(t, blocks) == 1 % blocks) & (t > blocks) & (t < lag_back + chunks))
        def _():
            spectral(lax.div(t - 1, blocks) - 1)

        @pl.when((t >= lag_back) & (t < lag_back + chunks))
        def _():
            backward(t - lag_back)

        @pl.when((t >= lag_grid) & (t < lag_grid + chunks))
        def _():
            to_grid(t - lag_grid)

        @pl.when((t >= lag_sum) & (t < lag_sum + chunks))
        def _():
            gather_sum(t - lag_sum)

        @pl.when((t >= lag_end) & (t < lag_end + chunks))
        def _():
            finish(t - lag_end)

        return carry

    lax.fori_loop(0, chunks + lag_end, one_step, 0)

    def drain(c, carry):
        lv, b = split(c)
        wait(wst.at[lv, : n_lat - 1, band(b), :], zs.at[c])
        wait(zin.at[lv, : n_lat - 1, band(b), :], bs.at[c])
        wait(xin.at[lv, : n_lon - 1, :, cells(b)], gs.at[c])
        wait(part.at[pl.ds(aligned(c * step, GROUP), step), :], ms.at[c])
        return carry

    lax.fori_loop(0, chunks, drain, 0)


def in_one_kernel(
    control, perturbs, static_input, lat_basis, local_spectrum, static_spectrum, static_weight
):
    mem_dev, levels = control.shape[:2]
    cells = control.shape[-1]
    n_lat, n_lon = lax.axis_size("lat"), lax.axis_size("lon")
    rows = NLAT // n_lat
    cols = cells // rows
    step = STEP_ROWS
    klat = lat_basis.shape[1]
    chunks = levels * rows // step
    plain = lambda a: jnp.moveaxis(a.reshape(mem_dev, levels, cells), 0, 1)
    ctrl, pert = plain(control), plain(perturbs)
    table = jnp.asarray(packed_table(n_lat))
    sizes = (levels, n_lat, n_lon, rows, cols, step)
    pair = 3 * LANES
    packed = GROUP // 2 * pair
    sems = lambda n: pltpu.SemaphoreType.DMA((n,))
    hbm = pl.BlockSpec(memory_space=pl.ANY)
    result = pl.pallas_call(
        functools.partial(kernel, sizes),
        out_shape=jax.ShapeDtypeStruct((levels, 1, cells), F32),
        in_specs=[hbm] * 7 + [pl.BlockSpec(memory_space=pltpu.SMEM)],
        out_specs=pl.BlockSpec(memory_space=pltpu.VMEM),
        scratch_shapes=[
            pltpu.VMEM((levels, n_lon, GROUP, cells), BF16),
            pltpu.VMEM((levels, n_lat, rows, packed), BF16),
            pltpu.VMEM((levels, n_lat, rows, packed), BF16),
            pltpu.VMEM((levels, n_lat, rows, packed), BF16),
            pltpu.VMEM((levels, n_lon, GROUP, cells), BF16),
            pltpu.VMEM(table.shape, BF16),
            pltpu.VMEM((n_lat, rows, klat), BF16),
            pltpu.VMEM((n_lat, klat, rows), BF16),
            pltpu.VMEM((2, klat, pair), F32),
            pltpu.VMEM((klat, packed), BF16),
            pltpu.VMEM((step * GROUP, NLON), BF16),
            pltpu.VMEM((table.shape[1] // LANES, step * GROUP, LANES), F32),
            pltpu.VMEM((step * GROUP, table.shape[1]), BF16),
            pltpu.VMEM((2, cols // LANES, step * GROUP, LANES), F32),
            pltpu.VMEM((2, mem_dev, step * cols), BF16),
            pltpu.VMEM((2, mem_dev, step * cols), BF16),
            pltpu.VMEM((levels, cells), BF16),
            pltpu.VMEM(local_spectrum.shape[::-1], F32),
            pltpu.VMEM(local_spectrum.shape[::-1], F32),
            pltpu.VMEM((levels * rows, cols), F32),
            pltpu.VMEM((levels * rows, cols), F32),
            sems(5),
            *[sems(chunks)] * 10,
            sems(2),
            sems(2),
        ],
        compiler_params=pltpu.CompilerParams(
            collective_id=0, has_side_effects=True, vmem_limit_bytes=67043328
        ),
        name="covariance",
    )(
        ctrl, pert, static_input.reshape(levels, cells), table,
        lat_basis.reshape(n_lat, rows, klat), local_spectrum.T, static_spectrum.T, static_weight,
    )
    return result.reshape(levels, 1, 1, cells)


def mul(spec, a, b):
    return jnp.einsum(spec, a, b, preferred_element_type=jnp.float32)


def by_waves(
    control, perturbs, static_input, lat_basis, local_spectrum, static_spectrum, static_weight
):
    mem_dev, levels = (control.shape[0], control.shape[1])
    cell_count = control.shape[-1]
    lat_rows = NLAT // lax.axis_size("lat")
    lon_cols = cell_count // lat_rows
    fields = jnp.concatenate([control, static_input[None]], 0).reshape(-1, lat_rows, lon_cols)
    per_lon = fields.shape[0] // lax.axis_size("lon")
    field_index = lax.axis_index("lon") * per_lon + jnp.arange(per_lon, dtype=jnp.int32)
    is_static = field_index >= mem_dev * levels
    first_mem = (lax.axis_index("mem") == 0).astype(jnp.float32)
    zonal = jnp.asarray(zonal_table())
    strips = lax.all_to_all(fields, "lon", split_axis=0, concat_axis=2, tiled=True)
    waves = mul("bxn,nk->kbx", strips, zonal).astype(jnp.bfloat16)
    merid = lax.all_to_all(waves, "lat", split_axis=0, concat_axis=2, tiled=True)
    coef = mul("kby,yj->kbj", merid, lat_basis)
    spectrum = jnp.where(
        is_static[None, :, None], static_spectrum.T[:, None, :], local_spectrum.T[:, None, :]
    )
    scaled = (coef * spectrum).astype(jnp.bfloat16)
    back = mul("kbj,yj->kby", scaled, lat_basis).astype(jnp.bfloat16)
    zonal_rows = lax.all_to_all(back, "lat", split_axis=2, concat_axis=0, tiled=True)
    grid = mul("kbx,nk->bxn", zonal_rows, zonal).astype(jnp.bfloat16)
    pert_fields = perturbs.reshape(mem_dev, levels, lat_rows, lon_cols)
    weight = static_weight[:, None, None]
    filtered = lax.all_to_all(grid, "lon", split_axis=2, concat_axis=0, tiled=True).reshape(
        mem_dev + 1, levels, lat_rows, lon_cols
    )
    ensemble = mul("mlxn,mlxn->lxn", pert_fields, filtered[:mem_dev])
    static_part = filtered[mem_dev].astype(jnp.float32)
    own = first_mem * weight * static_part + (1.0 - weight) * ensemble
    total = lax.psum(own, "mem")
    return total.reshape(levels, 1, 1, cell_count)


def fits(control):
    n_mem, n_lat, n_lon = (lax.axis_size(a) for a in ("mem", "lat", "lon"))
    rows = NLAT // n_lat
    cols = control.shape[-1] // rows
    return (
        n_mem == 2
        and control.shape[0] + 1 == GROUP * n_lon
        and KLON // n_lat == LANES + HALF
        and n_lat & (n_lat - 1) == 0
        and n_lon & (n_lon - 1) == 0
        and rows % STEP_ROWS == 0
        and cols % LANES == 0
        and rows // STEP_ROWS > 1
    )


def solution(mesh):
    def shards(control, *rest):
        body = in_one_kernel if fits(control) else by_waves
        return body(control, *rest)

    return jax.shard_map(
        shards,
        mesh=mesh,
        in_specs=(
            P("mem", None, "lat", "lon", None),
            P("mem", None, "lat", "lon", None),
            P(None, "lat", "lon", None),
            P(),
            P(None, "lat"),
            P(None, "lat"),
            P(),
        ),
        out_specs=P(None, "lat", "lon", None),
        check_vma=False,
    )
```

```python
import functools

import jax
import jax.numpy as jnp
import numpy as np
from jax import lax
from jax.experimental import pallas as pl
from jax.experimental.pallas import tpu as pltpu
from jax.sharding import PartitionSpec as P

NLON = 1536
NLAT = 768
KLON = 768
LANES = 128
HALF = 64
GROUP = 8
STEP_ROWS = 16
AHEAD = 4
MESH = pl.DeviceIdType.MESH
F32, BF16 = jnp.float32, jnp.bfloat16


def zonal_table():
    half = KLON // 2
    column = np.arange(KLON)
    wave = np.where(column < half, column, column - half + 1)
    angle = 2.0 * np.pi / NLON * (np.arange(NLON)[:, None] * wave[None, :] % NLON)
    values = np.where(column[None, :] < half, np.cos(angle), np.sin(angle))
    return (np.sqrt(2.0 / NLON) * values).astype(jnp.bfloat16)


def packed_table(n_lat):
    blocks = zonal_table().reshape(NLON, n_lat, KLON // n_lat)
    main = blocks[:, :, :LANES].reshape(NLON, -1)
    rest = blocks[:, :, LANES:]
    swapped = rest.reshape(NLON, n_lat // 2, 2, HALF)[:, :, ::-1]
    return np.concatenate([main, rest.reshape(NLON, -1), swapped.reshape(NLON, -1)], 1)


def aligned(start, to):
    return pl.multiple_of(start, to)


def kernel(
    sizes,
    ctrl, pert, static_in, table_in, merid_in, local_in, global_in, weight,
    part, peer,
    xin, wst, zin, bin_, gin, table, merid, merid_t, spec,
    scaled, rows_in, waves, rows_out, grid, cbuf, pbuf, static, local_t, global_t,
    csem, xs, xr, zs, zr, bs, br, gs, gr, ms, mr, cs, ps,
):
    levels, n_lat, n_lon, rows, cols, step = sizes
    blocks = rows // step
    chunks = levels * blocks
    width = step * cols
    pair = 3 * LANES
    pairs = GROUP // 2
    rest_a = n_lat * LANES
    rest_b = rest_a + n_lat * HALF
    my_mem, my_lat, my_lon = lax.axis_index("mem"), lax.axis_index("lat"), lax.axis_index("lon")
    lon_order = [2, 3, 1] if n_lon == 4 else list(range(1, n_lon))
    lat_order = [2, 3, 1] if n_lat == 4 else list(range(1, n_lat))

    def at_lon(lon):
        return (my_mem, my_lat, lon)

    def at_lat(lat):
        return (my_mem, lat, my_lon)

    def split(c):
        return lax.div(c, blocks), lax.rem(c, blocks)

    def cells(b):
        return pl.ds(aligned(b * width, LANES), width)

    def band(b):
        return pl.ds(aligned(b * step, 16), step)

    def remote(src, dst, send, recv, device):
        pltpu.make_async_remote_copy(
            src_ref=src, dst_ref=dst, send_sem=send, recv_sem=recv,
            device_id=device, device_id_type=MESH,
        ).start()

    def wait(ref, sem):
        pltpu.make_async_copy(ref, ref, sem).wait()

    tail = (n_lon - 1) * GROUP
    consts = [
        (static_in, static), (merid_in, merid), (local_in, local_t), (global_in, global_t),
        (table_in, table),
    ]
    for i, (src, dst) in enumerate(consts):
        pltpu.make_async_copy(src, dst, csem.at[i]).start()

    barrier = pltpu.get_barrier_semaphore()
    for s in range(1, n_lon):
        pl.semaphore_signal(barrier, 1, device_id=at_lon(my_lon ^ s), device_id_type=MESH)
    for s in range(1, n_lat):
        pl.semaphore_signal(barrier, 1, device_id=at_lat(my_lat ^ s), device_id_type=MESH)
    mem_peer = (1 - my_mem, my_lat, my_lon)
    pl.semaphore_signal(barrier, 1, device_id=mem_peer, device_id_type=MESH)
    pl.semaphore_wait(barrier, n_lon + n_lat - 1)

    def load_members(src, buf, sem, c):
        lv, b = split(c)
        slot = lax.rem(c, 2)
        return pltpu.make_async_copy(src.at[lv, :, cells(b)], buf.at[slot], sem.at[slot])

    def send_strips(c):
        lv, b = split(c)
        dst = xin.at[lv, my_lon, :, cells(b)]
        stage = gin.at[lv, my_lon, :, cells(b)]

        def strip(lon):
            return ctrl.at[lv, pl.ds(aligned(lon * GROUP, GROUP), GROUP), cells(b)]

        def send(src, lon):
            remote(src, dst, xs.at[c], xr.at[c], at_lon(lon))

        for s in lon_order:
            lon = my_lon ^ s

            @pl.when(lon < n_lon - 1)
            def _(lon=lon):
                send(strip(lon), lon)

        load_members(ctrl, cbuf, cs, c).wait()

        @pl.when(c + 1 < chunks)
        def _():
            load_members(ctrl, cbuf, cs, c + 1).start()

        def two_rows(i, carry):
            at = pl.ds(aligned(i * (2 * cols), LANES), 2 * cols)
            all_at = pl.ds(aligned(b * width + i * (2 * cols), LANES), 2 * cols)
            x = cbuf[lax.rem(c, 2), tail:, at].astype(F32)
            v = static[:, all_at].astype(F32)
            row = v[levels - 1 : levels]
            for k in range(levels - 1):
                row = jnp.where(lv == k, v[k : k + 1], row)
            gin[lv, my_lon, :, all_at] = jnp.concatenate([x, row], 0).astype(BF16)
            return carry

        lax.fori_loop(0, step // 2, two_rows, 0)

        @pl.when(my_lon < n_lon - 1)
        def _():
            send(stage, n_lon - 1)
            pltpu.make_async_copy(strip(my_lon), dst, xr.at[c]).start()

        @pl.when(my_lon == n_lon - 1)
        def _():
            pltpu.make_async_copy(stage, dst, xr.at[c]).start()

    load_members(ctrl, cbuf, cs, 0).start()
    load_members(pert, pbuf, ps, 0).start()
    pltpu.make_async_copy(static_in, static, csem.at[0]).wait()
    for c in range(min(AHEAD, chunks)):
        send_strips(c)
    for i, (src, dst) in enumerate(consts[1:]):
        pltpu.make_async_copy(src, dst, csem.at[i + 1]).wait()
    for d in range(n_lat):
        merid_t[d] = merid[d].astype(F32).T.astype(BF16)
    shared = jnp.where(my_lon == n_lon - 1, global_t[...], local_t[...])
    for kind, (even, odd) in enumerate([(local_t[...], local_t[...]), (local_t[...], shared)]):
        both = jnp.concatenate([even[:LANES], odd[:LANES], even[LANES:], odd[LANES:]], 0)
        spec[kind] = both.T

    low = lax.broadcasted_iota(jnp.int32, (step, LANES), 1) < HALF
    low_16 = low.astype(F32).astype(BF16)
    high_16 = (1.0 - low.astype(F32)).astype(BF16)

    def forward(c):
        lv, b = split(c)
        wait(xin.at[lv, :, :, cells(b)], xr.at[c])

        for i in range(step // 2):
            for e in range(n_lon):
                at = pl.ds(aligned(b * width + i * (2 * cols), LANES), 2 * cols)
                x = xin[lv, e, :, at].astype(F32)
                x = jnp.concatenate([x[:, :cols], x[:, cols:]], 0).astype(BF16)
                rows_in[i * 16 : (i + 1) * 16, e * cols : (e + 1) * cols] = x
        for k in range(0, waves.shape[0], 2):
            at = slice(k * LANES, (k + 2) * LANES)
            pair_k = jnp.dot(rows_in[...], table[:, at], preferred_element_type=F32)
            waves[k] = pair_k[:, :LANES]
            waves[k + 1] = pair_k[:, LANES:]
        for p in range(pairs):
            for d in range(n_lat):
                main = d
                in_a = rest_a // LANES + d // 2
                in_b = rest_b // LANES + d // 2
                first, second = (in_a, in_b) if d % 2 == 0 else (in_b, in_a)
                even, odd = pl.ds(2 * p, step, GROUP), pl.ds(2 * p + 1, step, GROUP)
                last = jnp.where(low, waves[first, even, :], waves[second, odd, :])
                at = p * pair
                wst[lv, d, band(b), at : at + LANES] = waves[main, even, :].astype(BF16)
                wst[lv, d, band(b), at + LANES : at + 2 * LANES] = waves[main, odd, :].astype(BF16)
                wst[lv, d, band(b), at + 2 * LANES : at + pair] = last.astype(BF16)
        dst = zin.at[lv, my_lat, band(b), :]
        for s in lat_order:
            lat = my_lat ^ s
            remote(wst.at[lv, lat, band(b), :], dst, zs.at[c], zr.at[c], at_lat(lat))
        pltpu.make_async_copy(wst.at[lv, my_lat, band(b), :], dst, zr.at[c]).start()

    def spectral(lv):
        def arrived(b, carry):
            wait(zin.at[lv, :, band(b), :], zr.at[lv * blocks + b])
            return carry

        lax.fori_loop(0, blocks, arrived, 0)
        for p in range(pairs):
            at = slice(p * pair, (p + 1) * pair)
            coef = sum(
                jnp.dot(merid_t[d], zin[lv, d, :, at], preferred_element_type=F32)
                for d in range(n_lat)
            )
            kind = 1 if p == pairs - 1 else 0
            scaled[:, at] = (coef * spec[kind]).astype(BF16)

    def backward(c):
        lv, b = split(c)
        lhs = jnp.concatenate([merid[d, band(b), :] for d in range(n_lat)], 0)
        for p in range(pairs):
            at = slice(p * pair, (p + 1) * pair)
            back = jnp.dot(lhs, scaled[:, at], preferred_element_type=F32).astype(BF16)
            for d in range(n_lat):
                zin[lv, d, band(b), at] = back[d * step : (d + 1) * step]
        dst = bin_.at[lv, my_lat, band(b), :]
        for s in lat_order:
            lat = my_lat ^ s
            remote(zin.at[lv, lat, band(b), :], dst, bs.at[c], br.at[c], at_lat(lat))
        pltpu.make_async_copy(zin.at[lv, my_lat, band(b), :], dst, br.at[c]).start()

    def to_grid(c):
        lv, b = split(c)
        wait(bin_.at[lv, :, band(b), :], br.at[c])
        for p in range(pairs):
            even = slice(2 * p * step, (2 * p + 1) * step)
            odd = slice((2 * p + 1) * step, (2 * p + 2) * step)
            at = p * pair
            for s in range(n_lat):
                main = slice(s * LANES, (s + 1) * LANES)
                in_a = slice(rest_a + s // 2 * LANES, rest_a + (s // 2 + 1) * LANES)
                in_b = slice(rest_b + s // 2 * LANES, rest_b + (s // 2 + 1) * LANES)
                first, second = (in_a, in_b) if s % 2 == 0 else (in_b, in_a)
                rest = bin_[lv, s, band(b), at + 2 * LANES : at + pair]
                rows_out[even, main] = bin_[lv, s, band(b), at : at + LANES]
                rows_out[odd, main] = bin_[lv, s, band(b), at + LANES : at + 2 * LANES]
                rows_out[even, first] = rest * low_16
                rows_out[odd, second] = rest * high_16
        wait(xin.at[lv, : n_lon - 1, :, cells(b)], xs.at[c])
        dst = gin.at[lv, my_lon, :, cells(b)]
        for turn, s in enumerate(lon_order + [0]):
            lon = my_lon ^ s
            strip = table[pl.ds(aligned(lon * cols, LANES), cols), :]
            part_e = lax.dot_general(
                rows_out[...], strip, (((1,), (1,)), ((), ())), preferred_element_type=F32
            )
            for m in range(GROUP):
                for j in range(cols // LANES):
                    tile = part_e[m * step : (m + 1) * step, j * LANES : (j + 1) * LANES]
                    grid[turn % 2, j, pl.ds(m, step, GROUP), :] = tile
            for i in range(step // 2):
                x = [
                    grid[turn % 2, j, i * 16 + h : i * 16 + h + GROUP, :]
                    for h in (0, GROUP)
                    for j in range(cols // LANES)
                ]
                at = pl.ds(aligned(b * width + i * (2 * cols), LANES), 2 * cols)
                xin[lv, lon, :, at] = jnp.concatenate(x, 1).astype(BF16)
            src = xin.at[lv, lon, :, cells(b)]
            if s:
                remote(src, dst, gs.at[c], gr.at[c], at_lon(lon))
            else:
                pltpu.make_async_copy(src, dst, gr.at[c]).start()

    owns = jnp.where(my_mem == 0, 1.0, 0.0).astype(F32)

    def gather_sum(c):
        lv, b = split(c)
        slot = lax.rem(c, 2)
        load_members(pert, pbuf, ps, c).wait()

        @pl.when(c + 1 < chunks)
        def _():
            load_members(pert, pbuf, ps, c + 1).start()

        wait(gin.at[lv, :, :, cells(b)], gr.at[c])
        w = weight[lv]

        def eight_rows(i, carry):
            for y in range(GROUP):
                off = aligned(i * (GROUP * cols) + y * cols, LANES)
                total = jnp.zeros((GROUP, cols), F32)
                here = pl.ds(off, cols)
                there = pl.ds(aligned(b * width + off, LANES), cols)
                for e in range(n_lon - 1):
                    factor = pbuf[slot, e * GROUP : (e + 1) * GROUP, here].astype(F32)
                    total += gin[lv, e, :, there].astype(F32) * factor
                field = gin[lv, n_lon - 1, :, there].astype(F32)
                last = field[: GROUP - 1] * pbuf[slot, tail:, here].astype(F32)
                total = (1.0 - w) * (jnp.sum(total, 0, keepdims=True) + jnp.sum(last, 0, keepdims=True))
                total += owns * w * field[GROUP - 1 :]
                part[lv, :, there] = total
            return carry

        lax.fori_loop(0, step // GROUP, eight_rows, 0)
        remote(part.at[lv, :, cells(b)], peer.at[lv, :, cells(b)], ms.at[c], mr.at[c], mem_peer)

    def finish(c):
        lv, b = split(c)
        wait(peer.at[lv, :, cells(b)], mr.at[c])

    lag_back = blocks + 1
    lag_grid = lag_back + 2
    lag_sum = lag_grid + 2
    lag_end = lag_sum + 1

    def one_step(t, carry):
        @pl.when(t + AHEAD < chunks)
        def _():
            send_strips(t + AHEAD)

        @pl.when(t < chunks)
        def _():
            forward(t)

        @pl.when((lax.rem(t, blocks) == 1 % blocks) & (t > blocks) & (t < lag_back + chunks))
        def _():
            spectral(lax.div(t - 1, blocks) - 1)

        @pl.when((t >= lag_back) & (t < lag_back + chunks))
        def _():
            backward(t - lag_back)

        @pl.when((t >= lag_grid) & (t < lag_grid + chunks))
        def _():
            to_grid(t - lag_grid)

        @pl.when((t >= lag_sum) & (t < lag_sum + chunks))
        def _():
            gather_sum(t - lag_sum)

        @pl.when((t >= lag_end) & (t < lag_end + chunks))
        def _():
            finish(t - lag_end)

        return carry

    lax.fori_loop(0, chunks + lag_end, one_step, 0)

    def drain(c, carry):
        lv, b = split(c)
        wait(wst.at[lv, : n_lat - 1, band(b), :], zs.at[c])
        wait(zin.at[lv, : n_lat - 1, band(b), :], bs.at[c])
        wait(xin.at[lv, : n_lon - 1, :, cells(b)], gs.at[c])
        wait(part.at[lv, :, cells(b)], ms.at[c])
        return carry

    lax.fori_loop(0, chunks, drain, 0)


def in_one_kernel(
    control, perturbs, static_input, lat_basis, local_spectrum, static_spectrum, static_weight
):
    mem_dev, levels = control.shape[:2]
    cells = control.shape[-1]
    n_lat, n_lon = lax.axis_size("lat"), lax.axis_size("lon")
    rows = NLAT // n_lat
    cols = cells // rows
    step = STEP_ROWS
    klat = lat_basis.shape[1]
    chunks = levels * rows // step
    plain = lambda a: jnp.moveaxis(a.reshape(mem_dev, levels, cells), 0, 1)
    ctrl, pert = plain(control), plain(perturbs)
    table = jnp.asarray(packed_table(n_lat))
    sizes = (levels, n_lat, n_lon, rows, cols, step)
    pair = 3 * LANES
    packed = GROUP // 2 * pair
    sems = lambda n: pltpu.SemaphoreType.DMA((n,))
    hbm = pl.BlockSpec(memory_space=pl.ANY)
    own, other = pl.pallas_call(
        functools.partial(kernel, sizes),
        out_shape=[jax.ShapeDtypeStruct((levels, 1, cells), F32)] * 2,
        in_specs=[hbm] * 7 + [pl.BlockSpec(memory_space=pltpu.SMEM)],
        out_specs=[pl.BlockSpec(memory_space=pltpu.VMEM)] * 2,
        scratch_shapes=[
            pltpu.VMEM((levels, n_lon, GROUP, cells), BF16),
            pltpu.VMEM((levels, n_lat, rows, packed), BF16),
            pltpu.VMEM((levels, n_lat, rows, packed), BF16),
            pltpu.VMEM((levels, n_lat, rows, packed), BF16),
            pltpu.VMEM((levels, n_lon, GROUP, cells), BF16),
            pltpu.VMEM(table.shape, BF16),
            pltpu.VMEM((n_lat, rows, klat), BF16),
            pltpu.VMEM((n_lat, klat, rows), BF16),
            pltpu.VMEM((2, klat, pair), F32),
            pltpu.VMEM((klat, packed), BF16),
            pltpu.VMEM((step * GROUP, NLON), BF16),
            pltpu.VMEM((table.shape[1] // LANES, step * GROUP, LANES), F32),
            pltpu.VMEM((step * GROUP, table.shape[1]), BF16),
            pltpu.VMEM((2, cols // LANES, step * GROUP, LANES), F32),
            pltpu.VMEM((2, mem_dev, step * cols), BF16),
            pltpu.VMEM((2, mem_dev, step * cols), BF16),
            pltpu.VMEM((levels, cells), BF16),
            pltpu.VMEM(local_spectrum.shape[::-1], F32),
            pltpu.VMEM(local_spectrum.shape[::-1], F32),
            sems(5),
            *[sems(chunks)] * 10,
            sems(2),
            sems(2),
        ],
        compiler_params=pltpu.CompilerParams(
            collective_id=0, has_side_effects=True, vmem_limit_bytes=67043328
        ),
        name="covariance",
    )(
        ctrl, pert, static_input.reshape(levels, cells), table,
        lat_basis.reshape(n_lat, rows, klat), local_spectrum.T, static_spectrum.T, static_weight,
    )
    return (own + other).reshape(levels, 1, 1, cells)


def mul(spec, a, b):
    return jnp.einsum(spec, a, b, preferred_element_type=jnp.float32)


def by_waves(
    control, perturbs, static_input, lat_basis, local_spectrum, static_spectrum, static_weight
):
    mem_dev, levels = (control.shape[0], control.shape[1])
    cell_count = control.shape[-1]
    lat_rows = NLAT // lax.axis_size("lat")
    lon_cols = cell_count // lat_rows
    fields = jnp.concatenate([control, static_input[None]], 0).reshape(-1, lat_rows, lon_cols)
    per_lon = fields.shape[0] // lax.axis_size("lon")
    field_index = lax.axis_index("lon") * per_lon + jnp.arange(per_lon, dtype=jnp.int32)
    is_static = field_index >= mem_dev * levels
    first_mem = (lax.axis_index("mem") == 0).astype(jnp.float32)
    zonal = jnp.asarray(zonal_table())
    strips = lax.all_to_all(fields, "lon", split_axis=0, concat_axis=2, tiled=True)
    waves = mul("bxn,nk->kbx", strips, zonal).astype(jnp.bfloat16)
    merid = lax.all_to_all(waves, "lat", split_axis=0, concat_axis=2, tiled=True)
    coef = mul("kby,yj->kbj", merid, lat_basis)
    spectrum = jnp.where(
        is_static[None, :, None], static_spectrum.T[:, None, :], local_spectrum.T[:, None, :]
    )
    scaled = (coef * spectrum).astype(jnp.bfloat16)
    back = mul("kbj,yj->kby", scaled, lat_basis).astype(jnp.bfloat16)
    zonal_rows = lax.all_to_all(back, "lat", split_axis=2, concat_axis=0, tiled=True)
    grid = mul("kbx,nk->bxn", zonal_rows, zonal).astype(jnp.bfloat16)
    pert_fields = perturbs.reshape(mem_dev, levels, lat_rows, lon_cols)
    weight = static_weight[:, None, None]
    filtered = lax.all_to_all(grid, "lon", split_axis=2, concat_axis=0, tiled=True).reshape(
        mem_dev + 1, levels, lat_rows, lon_cols
    )
    ensemble = mul("mlxn,mlxn->lxn", pert_fields, filtered[:mem_dev])
    static_part = filtered[mem_dev].astype(jnp.float32)
    own = first_mem * weight * static_part + (1.0 - weight) * ensemble
    total = lax.psum(own, "mem")
    return total.reshape(levels, 1, 1, cell_count)


def fits(control):
    n_mem, n_lat, n_lon = (lax.axis_size(a) for a in ("mem", "lat", "lon"))
    rows = NLAT // n_lat
    cols = control.shape[-1] // rows
    return (
        n_mem == 2
        and control.shape[0] + 1 == GROUP * n_lon
        and KLON // n_lat == LANES + HALF
        and n_lat & (n_lat - 1) == 0
        and n_lon & (n_lon - 1) == 0
        and rows % STEP_ROWS == 0
        and cols % LANES == 0
        and rows // STEP_ROWS > 1
    )


def solution(mesh):
    def shards(control, *rest):
        body = in_one_kernel if fits(control) else by_waves
        return body(control, *rest)

    return jax.shard_map(
        shards,
        mesh=mesh,
        in_specs=(
            P("mem", None, "lat", "lon", None),
            P("mem", None, "lat", "lon", None),
            P(None, "lat", "lon", None),
            P(),
            P(None, "lat"),
            P(None, "lat"),
            P(),
        ),
        out_specs=P(None, "lat", "lon", None),
        check_vma=False,
    )
```
